8 devices in a mesh: dp: 1 (over z), tp: 2 (over y), pp: 4 (over x, core).
Axes of the slice: x: 2, y: 2, z: 1, core: 2. Of those that a mesh axis runs over, the one named last changes fastest.
Arguments:
- hidden_in: bfloat16 [8, 1, 768, 2048], P('dp', None, 'tp')
- norm_gains: float32 [4, 4, 2048], P('pp')
- w_query: bfloat16 [4, 2048, 8, 256], P('pp', None, 'tp')
- w_key: bfloat16 [4, 2048, 2, 256], P('pp')
- w_value: bfloat16 [4, 2048, 2, 256], P('pp')
- w_out: bfloat16 [4, 8, 256, 2048], P('pp', 'tp')
- w_gate: bfloat16 [4, 2048, 16384], P('pp', None, 'tp')
- w_up: bfloat16 [4, 2048, 16384], P('pp', None, 'tp')
- w_down: bfloat16 [4, 16384, 2048], P('pp', 'tp')
Outputs:
- output: bfloat16 [8, 1, 768, 2048], P('dp', None, ('tp', 'pp'))
All inputs are finite; a program needn't handle non-finite values.
Results may differ from the reference program's by a relative error of at most 0.02.
Values are sent between devices in bfloat16 or wider.
A program may use at most 1 GiB of HBM per device.

```python
import jax
import jax.numpy as jnp
from jax import lax

D = 2048
HEADS = 8
KV_HEADS = 2
HEAD = 256
FF = 16384
WINDOW = 512
MICRO = 8
BATCH = 1
SEQ = 768
LAYERS = 4
SOFTCAP = 50
ROPE_BASE = 10000
Q_BLOCK = 256
NORM_EPS = 1e-6


def setup_inputs(seed: int = 0, part: int = 0) -> dict:
    root = jax.random.key(seed)
    part_key = jax.random.fold_in(jax.random.fold_in(root, 1), part)
    layer_keys = jax.random.split(jax.random.fold_in(root, 2), 8)

    def weight(rng_key, array_shape, fan_in):
        return (jax.random.normal(rng_key, array_shape, jnp.float32) * fan_in ** -0.5).astype(jnp.bfloat16)

    return {
        'hidden_in': jax.random.normal(part_key, (MICRO, BATCH, SEQ, D), jnp.float32).astype(jnp.bfloat16),
        'norm_gains': 0.4 * jax.random.normal(layer_keys[0], (LAYERS, 4, D), jnp.float32),
        'w_query': weight(layer_keys[1], (LAYERS, D, HEADS, HEAD), D),
        'w_key': weight(layer_keys[2], (LAYERS, D, KV_HEADS, HEAD), D),
        'w_value': weight(layer_keys[3], (LAYERS, D, KV_HEADS, HEAD), D),
        'w_out': weight(layer_keys[4], (LAYERS, HEADS, HEAD, D), HEADS * HEAD),
        'w_gate': weight(layer_keys[5], (LAYERS, D, FF), D),
        'w_up': weight(layer_keys[6], (LAYERS, D, FF), D),
        'w_down': weight(layer_keys[7], (LAYERS, FF, D), FF),
    }


def rms_scale(values, gain):
    as_f32 = values.astype(jnp.float32)
    mean_sq = jnp.mean(as_f32 * as_f32, axis=-1, keepdims=True)
    return (as_f32 * lax.rsqrt(mean_sq + NORM_EPS) * (1.0 + gain)).astype(jnp.bfloat16)


def apply_rope(projected):
    half_dim = HEAD // 2
    frequency = jnp.power(float(ROPE_BASE), -2.0 * jnp.arange(half_dim, dtype=jnp.float32) / HEAD)
    angle = jnp.arange(SEQ, dtype=jnp.float32)[:, None] * frequency[None, :]
    cos_t = jnp.cos(angle)[:, None, :]
    sin_t = jnp.sin(angle)[:, None, :]
    first = projected[..., :half_dim]
    second = projected[..., half_dim:]
    return jnp.concatenate([first * cos_t - second * sin_t, second * cos_t + first * sin_t], axis=-1).astype(jnp.bfloat16)


def attention(query, keys, values, is_local):
    group = HEADS // KV_HEADS
    grouped = query.reshape(SEQ, KV_HEADS, group, HEAD).astype(jnp.float32)
    key_f32 = keys.astype(jnp.float32)
    value_f32 = values.astype(jnp.float32)
    key_pos = jnp.arange(SEQ)
    scale = HEAD ** -0.5

    def one_block(start):
        q_part = lax.dynamic_slice_in_dim(grouped, start, Q_BLOCK, axis=0)
        scores = jnp.einsum('qkgd,skd->kgqs', q_part, key_f32) * scale
        scores = SOFTCAP * jnp.tanh(scores / SOFTCAP)
        offset = (start + jnp.arange(Q_BLOCK))[:, None] - key_pos[None, :]
        allowed = (offset >= 0) & ((offset < WINDOW) | jnp.logical_not(is_local))
        scores = jnp.where(allowed, scores, -1e30)
        attn_prob = jax.nn.softmax(scores, axis=-1).astype(jnp.bfloat16)
        mixed = jnp.einsum('kgqs,skd->qkgd', attn_prob.astype(jnp.float32), value_f32)
        return mixed.astype(jnp.bfloat16).reshape(Q_BLOCK, HEADS * HEAD)

    starts = jnp.arange(SEQ // Q_BLOCK) * Q_BLOCK
    return lax.map(one_block, starts).reshape(SEQ, HEADS * HEAD)


def apply_layer(residual, params):
    gains, w_q, w_k, w_v, w_o, w_g, w_u, w_d, index = params
    is_local = (index % 2) == 0
    normed = rms_scale(residual, gains[0])
    query = apply_rope(jnp.dot(normed, w_q.reshape(D, HEADS * HEAD), preferred_element_type=jnp.float32).reshape(SEQ, HEADS, HEAD))
    keys = apply_rope(jnp.dot(normed, w_k.reshape(D, KV_HEADS * HEAD), preferred_element_type=jnp.float32).reshape(SEQ, KV_HEADS, HEAD))
    values = jnp.dot(normed, w_v.reshape(D, KV_HEADS * HEAD), preferred_element_type=jnp.float32).astype(jnp.bfloat16).reshape(SEQ, KV_HEADS, HEAD)
    mixed = attention(query, keys, values, is_local)
    attn_proj = jnp.dot(mixed, w_o.reshape(HEADS * HEAD, D), preferred_element_type=jnp.float32).astype(jnp.bfloat16)
    residual = (residual.astype(jnp.float32) + rms_scale(attn_proj, gains[1]).astype(jnp.float32)).astype(jnp.bfloat16)
    normed = rms_scale(residual, gains[2])
    gate_proj = jnp.dot(normed, w_g, preferred_element_type=jnp.float32)
    up_proj = jnp.dot(normed, w_u, preferred_element_type=jnp.float32)
    hidden = (jax.nn.gelu(gate_proj, approximate=True) * up_proj).astype(jnp.bfloat16)
    down_proj = jnp.dot(hidden, w_d, preferred_element_type=jnp.float32).astype(jnp.bfloat16)
    return (residual.astype(jnp.float32) + rms_scale(down_proj, gains[3]).astype(jnp.float32)).astype(jnp.bfloat16)


def run_sequence(sequence, stacked):
    def layer_step(carry, params):
        return apply_layer(carry, params), None

    result, _ = lax.scan(layer_step, sequence, stacked)
    return result


def reference(hidden_in, norm_gains, w_query, w_key, w_value, w_out, w_gate, w_up, w_down):
    stacked = (norm_gains, w_query, w_key, w_value, w_out, w_gate, w_up, w_down, jnp.arange(LAYERS))
    sequences = hidden_in.reshape(MICRO * BATCH, SEQ, D)
    results = lax.map(lambda sequence: run_sequence(sequence, stacked), sequences)
    return results.reshape(MICRO, BATCH, SEQ, D)
```

```python
import functools

import jax
import jax.numpy as jnp
from jax import lax
from jax.experimental import pallas as pl
from jax.experimental.pallas import tpu as pltpu
from jax.sharding import PartitionSpec as P

WINDOW = 512
SOFTCAP = 50.0
ROPE_BASE = 10000.0
NORM_EPS = 1e-6
MESH = pl.DeviceIdType.MESH

D = 2048
HEAD = 256
HEADS = 8
KV = 2
GROUP = 4
FF_LOCAL = 8192
SEQ = 768
MICRO = 8
STAGES = 4
CHUNK = 192
CHUNKS = SEQ // CHUNK
ROWS = 2 * CHUNK
UNITS = (MICRO // 2) * CHUNKS
GATE_N = 512
GATE_BLOCKS = FF_LOCAL // GATE_N
DOWN_N = 256
DOWN_BLOCKS = D // DOWN_N
RING = 2
STRIP = 32
OUT_ROWS = 96
F32 = jnp.float32
BF16 = jnp.bfloat16


def rope_tables():
    half = HEAD // 2
    frequency = jnp.power(ROPE_BASE, -2.0 * jnp.arange(half, dtype=F32) / HEAD)
    angle = jnp.arange(SEQ, dtype=F32)[:, None] * frequency[None, :]
    return jnp.cos(angle), jnp.sin(angle)


def dot(a, b):
    return jnp.dot(a, b, preferred_element_type=F32)


def kernel(hidden, gains, cos, sin, wq_hbm, wkv_hbm, wo_hbm, wg_hbm, wu_hbm, wd_hbm, out,
           wq, wkv, wo, hid, wg, wu, wd, ubuf, kcache, vcache, xbuf, x1buf, psend, precv, acc,
           qbuf, hbuf, xout,
           load_sem, gq_sem, go_sem, g_sem, d_sem, u_send, u_recv, p_send, p_recv,
           x_recv, x_send, f_send, credit, go, out_recv, out_send, out_local):
    tp = lax.axis_index('tp')
    stage = lax.axis_index('pp')
    other = 1 - tp
    first = stage == 0
    last = stage == STAGES - 1
    odd = stage % 2
    half = HEADS // 2 * HEAD

    def g_copies(index):
        block = lax.rem(index, GATE_BLOCKS)
        slot = lax.rem(index, RING)
        cols = pl.ds(pl.multiple_of(block * GATE_N, GATE_N), GATE_N)
        return (pltpu.make_async_copy(wg_hbm.at[:, cols], wg.at[slot], g_sem.at[0, slot]),
                pltpu.make_async_copy(wu_hbm.at[:, cols], wu.at[slot], g_sem.at[1, slot]))

    def d_copy(index):
        block = lax.rem(index, DOWN_BLOCKS)
        slot = lax.rem(index, RING)
        cols = pl.ds(pl.multiple_of(block * DOWN_N, DOWN_N), DOWN_N)
        return pltpu.make_async_copy(wd_hbm.at[:, cols], wd.at[slot], d_sem.at[slot])

    def feed(unit):
        micro = lax.div(unit, CHUNKS)
        chunk = lax.rem(unit, CHUNKS)
        slot = lax.rem(unit, 2)

        @pl.when(first & (lax.div(chunk, 2) == tp))
        def _():
            rows = pl.ds(pl.multiple_of(lax.rem(chunk, 2) * CHUNK, CHUNK), CHUNK)
            pltpu.make_async_copy(hidden.at[2 * micro + tp, rows, :], xbuf.at[slot], x_recv.at[slot]).start()
            pltpu.make_async_remote_copy(
                hidden.at[2 * micro + other, rows, :], xbuf.at[slot], f_send.at[slot], x_recv.at[slot],
                device_id={'tp': other}, device_id_type=MESH).start()

    def feed_wait(unit):
        chunk = lax.rem(unit, CHUNKS)
        slot = lax.rem(unit, 2)

        @pl.when(first & (lax.div(chunk, 2) == tp))
        def _():
            pltpu.make_async_remote_copy(
                hidden.at[0, pl.ds(0, CHUNK), :], xbuf.at[slot], f_send.at[slot], x_recv.at[slot],
                device_id={'tp': other}, device_id_type=MESH).wait_send()

    gather_q = pltpu.make_async_remote_copy(
        wq_hbm, wq.at[:, pl.ds(pl.multiple_of(tp * half, half), half)], gq_sem.at[0], gq_sem.at[1],
        device_id={'tp': other}, device_id_type=MESH)
    gather_o = pltpu.make_async_remote_copy(
        wo_hbm, wo.at[pl.ds(pl.multiple_of(tp * half, half), half), :], go_sem.at[0], go_sem.at[1],
        device_id={'tp': other}, device_id_type=MESH)
    own_q = pltpu.make_async_copy(wq_hbm, wq.at[:, pl.ds(pl.multiple_of(tp * half, half), half)], load_sem.at[0])
    own_o = pltpu.make_async_copy(wo_hbm, wo.at[pl.ds(pl.multiple_of(tp * half, half), half), :], load_sem.at[1])
    own_kv = pltpu.make_async_copy(wkv_hbm, wkv, load_sem.at[2])

    def u_copy(unit):
        slot = lax.rem(unit, 2)
        return pltpu.make_async_remote_copy(
            ubuf.at[slot, pl.ds(0, CHUNK), :], ubuf.at[slot, pl.ds(CHUNK, CHUNK), :], u_send.at[slot], u_recv.at[slot],
            device_id={'tp': other}, device_id_type=MESH)

    def p_copy(unit, block):
        slot = lax.rem(unit, 2)
        cols = pl.ds(pl.multiple_of(block * DOWN_N, DOWN_N), DOWN_N)
        return pltpu.make_async_remote_copy(
            psend.at[:, cols], precv.at[slot, :, cols], p_send.at[block], p_recv.at[slot, block],
            device_id={'tp': other}, device_id_type=MESH)

    def x_copy(unit):
        slot = lax.rem(unit, 2)
        return pltpu.make_async_remote_copy(
            xout, xbuf.at[slot], x_send.at[slot], x_recv.at[slot],
            device_id={'pp': stage + 1}, device_id_type=MESH)

    def out_parts(unit):
        micro = 2 * lax.div(unit, CHUNKS) + tp
        chunk = lax.rem(unit, CHUNKS)
        to_tp = lax.div(chunk, 2)
        parts = []
        for t in range(2):
            to_pp = lax.rem(chunk, 2) * 2 + t
            here = (to_tp == tp) & (to_pp == STAGES - 1)
            rows = pl.ds(t * OUT_ROWS, OUT_ROWS)
            local = pltpu.make_async_copy(xout.at[rows, :], out.at[micro], out_local)
            remote = pltpu.make_async_remote_copy(
                xout.at[rows, :], out.at[micro], out_send.at[t], out_recv.at[micro],
                device_id={'tp': to_tp, 'pp': to_pp}, device_id_type=MESH)
            parts.append((here, local, remote))
        return parts

    def sends_wait(unit):
        @pl.when(jnp.logical_not(last))
        def _():
            x_copy(unit).wait_send()

        @pl.when(last)
        def _():
            for here, local, remote in out_parts(unit):
                @pl.when(here)
                def _():
                    local.wait()

                @pl.when(jnp.logical_not(here))
                def _():
                    remote.wait_send()

    def normed(values, gain_row):
        mean_sq = jnp.mean(values * values, axis=-1, keepdims=True)
        return (values * lax.rsqrt(mean_sq + NORM_EPS) * (1.0 + gains[pl.ds(gain_row, 1), :])).astype(BF16)

    def attention(chunk, n):
        base = chunk * CHUNK
        row = lax.broadcasted_iota(jnp.int32, (GROUP, CHUNK, n), 1).reshape(GROUP * CHUNK, n) + base
        col = lax.broadcasted_iota(jnp.int32, (GROUP * CHUNK, n), 1)
        offset = row - col
        reach = jnp.where(odd == 0, WINDOW, SEQ)
        allowed = (offset >= 0) & (offset < reach)
        for g in range(KV):
            q = qbuf[pl.ds(g * GROUP, GROUP)].reshape(GROUP * CHUNK, HEAD)
            k = kcache[pl.ds(0, n), g * HEAD:(g + 1) * HEAD]
            v = vcache[pl.ds(0, n), g * HEAD:(g + 1) * HEAD]
            s = lax.dot_general(q, k, (((1,), (1,)), ((), ())), preferred_element_type=F32)
            s = SOFTCAP * jnp.tanh(s * (HEAD ** -0.5 / SOFTCAP))
            e = jnp.where(allowed, jnp.exp(s), 0.0)
            p = (e / jnp.sum(e, axis=-1, keepdims=True)).astype(BF16)
            o = dot(p, v).astype(BF16)
            for h in range(GROUP):
                hbuf[:, (g * GROUP + h) * HEAD:(g * GROUP + h + 1) * HEAD] = o[h * CHUNK:(h + 1) * CHUNK, :]

    def attend(unit):
        chunk = lax.rem(unit, CHUNKS)
        slot = lax.rem(unit, 2)
        pltpu.make_async_copy(xout, xbuf.at[slot], x_recv.at[slot]).wait()

        @pl.loop(0, CHUNK // STRIP)
        def _(r):
            rows = pl.ds(pl.multiple_of(r * STRIP, STRIP), STRIP)
            hbuf[rows, :] = normed(xbuf[slot, rows, :].astype(F32), 0)

        @pl.when(unit == 0)
        def _():
            own_kv.wait()

        positions = pl.ds(pl.multiple_of(chunk * CHUNK, CHUNK), CHUNK)

        def rotated(value):
            a, b = value[:, :HEAD // 2], value[:, HEAD // 2:]
            c, s = cos[positions, :], sin[positions, :]
            return (a * c - b * s).astype(BF16), (b * c + a * s).astype(BF16)

        k = dot(hbuf[...], wkv[:, :KV * HEAD])
        for g in range(KV):
            a, b = rotated(k[:, g * HEAD:(g + 1) * HEAD])
            kcache[positions, g * HEAD:g * HEAD + HEAD // 2] = a
            kcache[positions, g * HEAD + HEAD // 2:(g + 1) * HEAD] = b
        vcache[positions, :] = dot(hbuf[...], wkv[:, KV * HEAD:]).astype(BF16)

        @pl.when(unit == 0)
        def _():
            own_q.wait()
            gather_q.wait()

        @pl.loop(0, HEADS // 2)
        def _(pair):
            q = dot(hbuf[...], wq[:, pl.ds(pl.multiple_of(pair * 2 * HEAD, 2 * HEAD), 2 * HEAD)])
            for t in range(2):
                a, b = rotated(q[:, t * HEAD:(t + 1) * HEAD])
                qbuf[pair * 2 + t, :, :HEAD // 2] = a
                qbuf[pair * 2 + t, :, HEAD // 2:] = b

        for c in range(CHUNKS):
            @pl.when(chunk == c)
            def _():
                attention(c, (c + 1) * CHUNK)

        @pl.when(unit == 0)
        def _():
            own_o.wait()
            gather_o.wait()

            @pl.when(odd == 0)
            def _():
                pl.semaphore_signal(go, 1, device_id={'pp': stage + 1}, device_id_type=MESH)

        @pl.loop(0, D // 512)
        def _(n):
            cols = pl.ds(pl.multiple_of(n * 512, 512), 512)
            acc[:, cols] = dot(hbuf[...], wo[:, cols])

        @pl.when(unit >= 2)
        def _():
            u_copy(unit).wait_send()

        @pl.loop(0, CHUNK // STRIP)
        def _(r):
            rows = pl.ds(pl.multiple_of(r * STRIP, STRIP), STRIP)
            branch = normed(acc[rows, :].astype(BF16).astype(F32), 1)
            x1 = (xbuf[slot, rows, :].astype(F32) + branch.astype(F32)).astype(BF16)
            x1buf[slot, rows, :] = x1
            ubuf[slot, rows, :] = normed(x1.astype(F32), 2)

        u_copy(unit).start()

        @pl.when(jnp.logical_not(first) & (unit < UNITS - 2))
        def _():
            pl.semaphore_signal(credit, 1, device_id={'pp': stage - 1}, device_id_type=MESH)

    def gate_up(unit):
        slot = lax.rem(unit, 2)
        u_copy(unit).wait_recv()

        @pl.when(unit + 2 < UNITS)
        def _():
            feed_wait(unit)
            feed(unit + 2)

        @pl.loop(0, GATE_BLOCKS)
        def _(block):
            index = unit * GATE_BLOCKS + block
            ring = lax.rem(index, RING)
            for copy in g_copies(index):
                copy.wait()
            for t in range(GATE_N // 256):
                sub = slice(t * 256, (t + 1) * 256)
                gate = dot(ubuf[slot], wg[ring, :, sub])
                up = dot(ubuf[slot], wu[ring, :, sub])
                hid[:, pl.ds(pl.multiple_of(block * GATE_N + t * 256, 256), 256)] = (
                    jax.nn.gelu(gate, approximate=True) * up).astype(BF16)

            @pl.when(index + RING < UNITS * GATE_BLOCKS)
            def _():
                for copy in g_copies(index + RING):
                    copy.start()

    def down(unit):
        @pl.loop(0, DOWN_BLOCKS)
        def _(block):
            index = unit * DOWN_BLOCKS + block
            ring = lax.rem(index, RING)
            cols = pl.ds(pl.multiple_of(block * DOWN_N, DOWN_N), DOWN_N)
            d_copy(index).wait()

            @pl.when(unit > 0)
            def _():
                p_copy(unit, block).wait_send()

            part = dot(hid[...], wd[ring])
            psend[:, cols] = part[CHUNK:, :].astype(BF16)
            acc[:, cols] = part[:CHUNK, :]
            p_copy(unit, block).start()

            @pl.when(index + RING < UNITS * DOWN_BLOCKS)
            def _():
                d_copy(index + RING).start()

    def finish(unit):
        slot = lax.rem(unit, 2)

        @pl.when(unit > 0)
        def _():
            sends_wait(unit - 1)

        @pl.loop(0, DOWN_BLOCKS)
        def _(block):
            p_copy(unit, block).wait_recv()

        @pl.loop(0, CHUNK // STRIP)
        def _(r):
            rows = pl.ds(pl.multiple_of(r * STRIP, STRIP), STRIP)
            total = (acc[rows, :] + precv[slot, rows, :].astype(F32)).astype(BF16)
            branch = normed(total.astype(F32), 3)
            xout[rows, :] = (x1buf[slot, rows, :].astype(F32) + branch.astype(F32)).astype(BF16)

        @pl.when(jnp.logical_not(last))
        def _():
            @pl.when(unit >= 2)
            def _():
                pl.semaphore_wait(credit, 1)
            x_copy(unit).start()

        @pl.when(last)
        def _():
            for here, local, remote in out_parts(unit):
                @pl.when(here)
                def _():
                    local.start()

                @pl.when(jnp.logical_not(here))
                def _():
                    remote.start()

    feed(0)
    own_kv.start()
    own_q.start()
    own_o.start()

    @pl.when(odd == 1)
    def _():
        pl.semaphore_wait(go, 1)

    gather_q.start()
    gather_o.start()
    feed(1)
    for s in range(RING):
        for copy in g_copies(s):
            copy.start()
        d_copy(s).start()

    attend(0)

    @pl.loop(0, UNITS)
    def _(unit):
        gate_up(unit)

        @pl.when(unit + 1 < UNITS)
        def _():
            attend(unit + 1)

        down(unit)
        finish(unit)

    sends_wait(UNITS - 1)
    feed_wait(UNITS - 2)
    feed_wait(UNITS - 1)
    for s in range(2):
        u_copy(UNITS - 2 + s).wait_send()

    @pl.loop(0, DOWN_BLOCKS)
    def _(block):
        p_copy(UNITS - 1, block).wait_send()

    for m in range(MICRO):
        @pl.when(jnp.logical_not(last & (tp == m % 2)))
        def _():
            pltpu.make_async_copy(xout.at[pl.ds(0, OUT_ROWS), :], out.at[m], out_recv.at[m]).wait()


def solution(mesh):
    in_specs = (P('dp', None, 'tp', None), P('pp', None, None), P('pp', None, 'tp', None),
                P('pp', None, None, None), P('pp', None, None, None), P('pp', 'tp', None, None),
                P('pp', None, 'tp'), P('pp', None, 'tp'), P('pp', 'tp', None))
    out_spec = P('dp', None, ('tp', 'pp'), None)

    def stage_program(hidden_in, norm_gains, w_query, w_key, w_value, w_out, w_gate, w_up, w_down):
        cos, sin = rope_tables()
        wq = w_query[0].reshape(D, HEADS // 2 * HEAD)
        wkv = jnp.concatenate([w_key[0].reshape(D, KV * HEAD), w_value[0].reshape(D, KV * HEAD)], axis=1)
        wo = w_out[0].reshape(HEADS // 2 * HEAD, D)
        hbm = pl.BlockSpec(memory_space=pl.ANY)
        vmem = pl.BlockSpec(memory_space=pltpu.VMEM)
        dma = pltpu.SemaphoreType.DMA
        out = pl.pallas_call(
            kernel,
            out_shape=jax.ShapeDtypeStruct((MICRO, OUT_ROWS, D), BF16),
            in_specs=[hbm, vmem, vmem, vmem] + [hbm] * 6,
            out_specs=hbm,
            scratch_shapes=[
                pltpu.VMEM((D, HEADS * HEAD), BF16),
                pltpu.VMEM((D, 2 * KV * HEAD), BF16),
                pltpu.VMEM((HEADS * HEAD, D), BF16),
                pltpu.VMEM((ROWS, FF_LOCAL), BF16),
                pltpu.VMEM((RING, D, GATE_N), BF16),
                pltpu.VMEM((RING, D, GATE_N), BF16),
                pltpu.VMEM((RING, FF_LOCAL, DOWN_N), BF16),
                pltpu.VMEM((2, ROWS, D), BF16),
                pltpu.VMEM((SEQ, KV * HEAD), BF16),
                pltpu.VMEM((SEQ, KV * HEAD), BF16),
                pltpu.VMEM((2, CHUNK, D), BF16),
                pltpu.VMEM((2, CHUNK, D), BF16),
                pltpu.VMEM((CHUNK, D), BF16),
                pltpu.VMEM((2, CHUNK, D), BF16),
                pltpu.VMEM((CHUNK, D), F32),
                pltpu.VMEM((HEADS, CHUNK, HEAD), BF16),
                pltpu.VMEM((CHUNK, D), BF16),
                pltpu.VMEM((CHUNK, D), BF16),
                dma((3,)), dma((2,)), dma((2,)), dma((2, RING)), dma((RING,)), dma((2,)), dma((2,)),
                dma((DOWN_BLOCKS,)), dma((2, DOWN_BLOCKS)), dma((2,)), dma((2,)), dma((2,)),
                pltpu.SemaphoreType.REGULAR, pltpu.SemaphoreType.REGULAR,
                dma((MICRO,)), dma((2,)), dma,
            ],
            compiler_params=pltpu.CompilerParams(has_side_effects=True, vmem_limit_bytes=67043328),
            name='pipeline',
        )(hidden_in.reshape(MICRO, SEQ // 2, D), norm_gains[0], cos, sin, wq, wkv, wo, w_gate[0], w_up[0], w_down[0])
        return out.reshape(MICRO, 1, OUT_ROWS, D)

    return jax.shard_map(stage_program, mesh=mesh, in_specs=in_specs, out_specs=out_spec, check_vma=False)
```

```python
import functools

import jax
import jax.numpy as jnp
from jax import lax
from jax.experimental import pallas as pl
from jax.experimental.pallas import tpu as pltpu
from jax.sharding import PartitionSpec as P

WINDOW = 512
SOFTCAP = 50.0
ROPE_BASE = 10000.0
NORM_EPS = 1e-6
MESH = pl.DeviceIdType.MESH

D = 2048
HEAD = 256
HEADS = 8
KV = 2
GROUP = 4
FF_LOCAL = 8192
SEQ = 768
MICRO = 8
STAGES = 4
CHUNK = 192
CHUNKS = SEQ // CHUNK
ROWS = 2 * CHUNK
UNITS = (MICRO // 2) * CHUNKS
GATE_N = 512
GATE_BLOCKS = FF_LOCAL // GATE_N
DOWN_N = 512
DOWN_BLOCKS = D // DOWN_N
DOWN_K = FF_LOCAL // D
RING = 8
FINISH_AT = 4
ATTEND_AT = 8
STRIP = 64
OUT_ROWS = 96
PIECES = 8
F32 = jnp.float32
BF16 = jnp.bfloat16


def rope_tables():
    half = HEAD // 2
    frequency = jnp.power(ROPE_BASE, -2.0 * jnp.arange(half, dtype=F32) / HEAD)
    angle = jnp.arange(SEQ, dtype=F32)[:, None] * frequency[None, :]
    return jnp.cos(angle), jnp.sin(angle)


def dot(a, b):
    return jnp.dot(a, b, preferred_element_type=F32)


def kernel(hidden, gains, cos, sin, wq_hbm, wkv_hbm, wo_hbm, wg_hbm, wu_hbm, wd_hbm, out,
           wq, wkv, wo, hid, ring, ubuf, kcache, vcache, xbuf, x1buf, psend, precv, acc,
           qbuf, hbuf, xout,
           load_sem, gq_sem, go_sem, relay_send, relay_recv, back_send, back_recv, ready, ring_sem, u_send, u_recv, p_send, p_recv,
           x_recv, x_send, f_send, credit, go, out_recv, out_send, out_local):
    tp = lax.axis_index('tp')
    stage = lax.axis_index('pp')
    other = 1 - tp
    first = stage == 0
    last = stage == STAGES - 1
    odd = stage % 2
    half = HEADS // 2 * HEAD
    west = stage < STAGES // 2
    piece = half // PIECES

    def gate_copies(block):
        slot = 2 * lax.rem(block, RING // 2)
        cols = pl.ds(pl.multiple_of(block * GATE_N, GATE_N), GATE_N)
        return (pltpu.make_async_copy(wg_hbm.at[:, cols], ring.at[slot], ring_sem.at[slot]),
                pltpu.make_async_copy(wu_hbm.at[:, cols], ring.at[slot + 1], ring_sem.at[slot + 1]))

    def down_copies(block, parts):
        slot = DOWN_K * lax.rem(block, RING // DOWN_K)
        cols = pl.ds(pl.multiple_of(block * DOWN_N, DOWN_N), DOWN_N)
        return [pltpu.make_async_copy(
            wd_hbm.at[pl.ds(part * D if isinstance(part, int) else pl.multiple_of(part * D, D), D), cols],
            ring.at[slot + part], ring_sem.at[slot + part]) for part in parts]

    def feed(unit):
        micro = lax.div(unit, CHUNKS)
        chunk = lax.rem(unit, CHUNKS)
        slot = lax.rem(unit, 2)

        @pl.when(first & (lax.div(chunk, 2) == tp))
        def _():
            rows = pl.ds(pl.multiple_of(lax.rem(chunk, 2) * CHUNK, CHUNK), CHUNK)
            pltpu.make_async_copy(hidden.at[2 * micro + tp, rows, :], xbuf.at[slot], x_recv.at[slot]).start()
            pltpu.make_async_remote_copy(
                hidden.at[2 * micro + other, rows, :], xbuf.at[slot], f_send.at[slot], x_recv.at[slot],
                device_id={'tp': other}, device_id_type=MESH).start()

    def feed_wait(unit):
        chunk = lax.rem(unit, CHUNKS)
        slot = lax.rem(unit, 2)

        @pl.when(first & (lax.div(chunk, 2) == tp))
        def _():
            pltpu.make_async_remote_copy(
                hidden.at[0, pl.ds(0, CHUNK), :], xbuf.at[slot], f_send.at[slot], x_recv.at[slot],
                device_id={'tp': other}, device_id_type=MESH).wait_send()

    gather_q = pltpu.make_async_remote_copy(
        wq_hbm, wq.at[:, pl.ds(pl.multiple_of(tp * half, half), half)], gq_sem.at[0], gq_sem.at[1],
        device_id={'tp': other}, device_id_type=MESH)
    gather_o = pltpu.make_async_remote_copy(
        wo_hbm, wo.at[pl.ds(pl.multiple_of(tp * half, half), half), :], go_sem.at[0], go_sem.at[1],
        device_id={'tp': other}, device_id_type=MESH)
    own_q = pltpu.make_async_copy(wq_hbm, wq.at[:, pl.ds(pl.multiple_of(tp * half, half), half)], load_sem.at[0])
    own_o = pltpu.make_async_copy(wo_hbm, wo.at[pl.ds(pl.multiple_of(tp * half, half), half), :], load_sem.at[1])
    own_kv = pltpu.make_async_copy(wkv_hbm, wkv, load_sem.at[2])

    def relay_out(p):
        rows = pl.ds(pl.multiple_of(p * piece, piece), piece)
        there = pl.ds(pl.multiple_of(tp * half + p * piece, piece), piece)
        return pltpu.make_async_remote_copy(
            wo_hbm.at[rows, :], wo.at[there, :], relay_send.at[p], relay_recv.at[p],
            device_id={'tp': other, 'pp': stage + STAGES // 2}, device_id_type=MESH)

    def relay_back(p):
        rows = pl.ds(pl.multiple_of(other * half + p * piece, piece), piece)
        return pltpu.make_async_remote_copy(
            wo.at[rows, :], wo.at[rows, :], back_send.at[p], back_recv.at[p],
            device_id={'pp': stage - STAGES // 2}, device_id_type=MESH)

    def gather_o_wait():
        own_o.wait()

        @pl.when(west)
        def _():
            @pl.loop(0, PIECES)
            def _(p):
                relay_out(p).wait_send()
                relay_back(p).wait_recv()

        @pl.when(jnp.logical_not(west))
        def _():
            gather_o.wait()

        @pl.when(odd == 0)
        def _():
            pl.semaphore_signal(go, 1, device_id={'pp': stage + 1}, device_id_type=MESH)

    def u_copy(unit):
        slot = lax.rem(unit, 2)
        return pltpu.make_async_remote_copy(
            ubuf.at[slot, pl.ds(0, CHUNK), :], ubuf.at[slot, pl.ds(CHUNK, CHUNK), :], u_send.at[slot], u_recv.at[slot],
            device_id={'tp': other}, device_id_type=MESH)

    def p_copy(unit, block):
        slot = lax.rem(unit, 2)
        cols = pl.ds(pl.multiple_of(block * DOWN_N, DOWN_N), DOWN_N)
        return pltpu.make_async_remote_copy(
            psend.at[:, cols], precv.at[slot, :, cols], p_send.at[block], p_recv.at[slot, block],
            device_id={'tp': other}, device_id_type=MESH)

    def x_copy(unit):
        slot = lax.rem(unit, 2)
        return pltpu.make_async_remote_copy(
            xout, xbuf.at[slot], x_send.at[slot], x_recv.at[slot],
            device_id={'pp': stage + 1}, device_id_type=MESH)

    def out_parts(unit):
        micro = 2 * lax.div(unit, CHUNKS) + tp
        chunk = lax.rem(unit, CHUNKS)
        to_tp = lax.div(chunk, 2)
        parts = []
        for t in range(2):
            to_pp = lax.rem(chunk, 2) * 2 + t
            here = (to_tp == tp) & (to_pp == STAGES - 1)
            rows = pl.ds(t * OUT_ROWS, OUT_ROWS)
            local = pltpu.make_async_copy(xout.at[rows, :], out.at[micro], out_local)
            remote = pltpu.make_async_remote_copy(
                xout.at[rows, :], out.at[micro], out_send.at[t], out_recv.at[micro],
                device_id={'tp': to_tp, 'pp': to_pp}, device_id_type=MESH)
            parts.append((here, local, remote))
        return parts

    def sends_wait(unit):
        @pl.when(jnp.logical_not(last))
        def _():
            x_copy(unit).wait_send()

        @pl.when(last)
        def _():
            for here, local, remote in out_parts(unit):
                @pl.when(here)
                def _():
                    local.wait()

                @pl.when(jnp.logical_not(here))
                def _():
                    remote.wait_send()

    def normed(values, gain_row):
        mean_sq = jnp.mean(values * values, axis=-1, keepdims=True)
        return (values * lax.rsqrt(mean_sq + NORM_EPS) * (1.0 + gains[pl.ds(gain_row, 1), :])).astype(BF16)

    def attention(chunk, n):
        base = chunk * CHUNK
        row = lax.broadcasted_iota(jnp.int32, (GROUP, CHUNK, n), 1).reshape(GROUP * CHUNK, n) + base
        col = lax.broadcasted_iota(jnp.int32, (GROUP * CHUNK, n), 1)
        offset = row - col
        reach = jnp.where(odd == 0, WINDOW, SEQ)
        allowed = (offset >= 0) & (offset < reach)
        for g in range(KV):
            q = qbuf[pl.ds(g * GROUP, GROUP)].reshape(GROUP * CHUNK, HEAD)
            k = kcache[pl.ds(0, n), g * HEAD:(g + 1) * HEAD]
            v = vcache[pl.ds(0, n), g * HEAD:(g + 1) * HEAD]
            s = lax.dot_general(q, k, (((1,), (1,)), ((), ())), preferred_element_type=F32)
            s = SOFTCAP * jnp.tanh(s * (HEAD ** -0.5 / SOFTCAP))
            e = jnp.where(allowed, jnp.exp(s), 0.0)
            p = (e / jnp.sum(e, axis=-1, keepdims=True)).astype(BF16)
            o = dot(p, v).astype(BF16)
            for h in range(GROUP):
                hbuf[:, (g * GROUP + h) * HEAD:(g * GROUP + h + 1) * HEAD] = o[h * CHUNK:(h + 1) * CHUNK, :]

    def attend(unit):
        chunk = lax.rem(unit, CHUNKS)
        slot = lax.rem(unit, 2)
        pltpu.make_async_copy(xout, xbuf.at[slot], x_recv.at[slot]).wait()

        @pl.loop(0, CHUNK // STRIP)
        def _(r):
            rows = pl.ds(pl.multiple_of(r * STRIP, STRIP), STRIP)
            hbuf[rows, :] = normed(xbuf[slot, rows, :].astype(F32), 0)

        @pl.when(unit == 0)
        def _():
            own_kv.wait()

        positions = pl.ds(pl.multiple_of(chunk * CHUNK, CHUNK), CHUNK)

        def rotated(value):
            a, b = value[:, :HEAD // 2], value[:, HEAD // 2:]
            c, s = cos[positions, :], sin[positions, :]
            return (a * c - b * s).astype(BF16), (b * c + a * s).astype(BF16)

        kv = dot(hbuf[...], wkv[...])
        k = kv[:, :KV * HEAD]
        for g in range(KV):
            a, b = rotated(k[:, g * HEAD:(g + 1) * HEAD])
            kcache[positions, g * HEAD:g * HEAD + HEAD // 2] = a
            kcache[positions, g * HEAD + HEAD // 2:(g + 1) * HEAD] = b
        vcache[positions, :] = kv[:, KV * HEAD:].astype(BF16)

        @pl.when(first & (unit == 0))
        def _():
            own_q.wait()
            gather_q.wait()

        @pl.loop(0, KV)
        def _(g):
            q = dot(hbuf[...], wq[:, pl.ds(pl.multiple_of(g * GROUP * HEAD, GROUP * HEAD), GROUP * HEAD)])
            for t in range(GROUP):
                a, b = rotated(q[:, t * HEAD:(t + 1) * HEAD])
                qbuf[g * GROUP + t, :, :HEAD // 2] = a
                qbuf[g * GROUP + t, :, HEAD // 2:] = b

        for c in range(CHUNKS):
            @pl.when(chunk == c)
            def _():
                attention(c, (c + 1) * CHUNK)

        @pl.when(first & (unit == 0))
        def _():
            gather_o_wait()

        @pl.loop(0, D // 1024)
        def _(n):
            cols = pl.ds(pl.multiple_of(n * 1024, 1024), 1024)
            acc[:, cols] = dot(hbuf[...], wo[:, cols])

        @pl.when(unit >= 2)
        def _():
            u_copy(unit).wait_send()

        @pl.loop(0, CHUNK // STRIP)
        def _(r):
            rows = pl.ds(pl.multiple_of(r * STRIP, STRIP), STRIP)
            branch = normed(acc[rows, :].astype(BF16).astype(F32), 1)
            x1 = (xbuf[slot, rows, :].astype(F32) + branch.astype(F32)).astype(BF16)
            x1buf[slot, rows, :] = x1
            ubuf[slot, rows, :] = normed(x1.astype(F32), 2)

        u_copy(unit).start()

        @pl.when(jnp.logical_not(first) & (unit < UNITS - 2))
        def _():
            pl.semaphore_signal(credit, 1, device_id={'pp': stage - 1}, device_id_type=MESH)

    def gate_up(unit, begin, end):
        slot = lax.rem(unit, 2)

        @pl.loop(begin, end)
        def _(block):
            for copy in gate_copies(block):
                copy.wait()
            at = 2 * lax.rem(block, RING // 2)
            gate = dot(ubuf[slot], ring[at])
            up = dot(ubuf[slot], ring[at + 1])
            hid[:, pl.ds(pl.multiple_of(block * GATE_N, GATE_N), GATE_N)] = (
                jax.nn.gelu(gate, approximate=True) * up).astype(BF16)
            ahead = block + RING // 2

            @pl.when(ahead < GATE_BLOCKS)
            def _():
                for copy in gate_copies(ahead):
                    copy.start()

            @pl.when(ahead >= GATE_BLOCKS)
            def _():
                over = ahead - GATE_BLOCKS
                for copy in down_copies(lax.div(over, 2), [2 * lax.rem(over, 2), 2 * lax.rem(over, 2) + 1]):
                    copy.start()

    def down(unit):
        @pl.loop(0, DOWN_BLOCKS)
        def _(block):
            cols = pl.ds(pl.multiple_of(block * DOWN_N, DOWN_N), DOWN_N)
            at = DOWN_K * lax.rem(block, RING // DOWN_K)

            @pl.when(unit > 0)
            def _():
                p_copy(unit, block).wait_send()

            for copy in down_copies(block, range(DOWN_K)):
                copy.wait()
            part = dot(hid[:, :D], ring[at])
            for k in range(1, DOWN_K):
                part = part + dot(hid[:, k * D:(k + 1) * D], ring[at + k])
            psend[:, cols] = part[CHUNK:, :].astype(BF16)
            acc[:, cols] = part[:CHUNK, :]
            p_copy(unit, block).start()
            ahead = block + RING // DOWN_K

            @pl.when(ahead < DOWN_BLOCKS)
            def _():
                for copy in down_copies(ahead, range(DOWN_K)):
                    copy.start()

            @pl.when((ahead >= DOWN_BLOCKS) & (unit + 1 < UNITS))
            def _():
                for t in range(2):
                    for copy in gate_copies((ahead - DOWN_BLOCKS) * 2 + t):
                        copy.start()

    def finish(unit):
        slot = lax.rem(unit, 2)

        @pl.when(unit > 0)
        def _():
            sends_wait(unit - 1)

        @pl.loop(0, DOWN_BLOCKS)
        def _(block):
            p_copy(unit, block).wait_recv()

        @pl.loop(0, CHUNK // STRIP)
        def _(r):
            rows = pl.ds(pl.multiple_of(r * STRIP, STRIP), STRIP)
            total = (acc[rows, :] + precv[slot, rows, :].astype(F32)).astype(BF16)
            branch = normed(total.astype(F32), 3)
            xout[rows, :] = (x1buf[slot, rows, :].astype(F32) + branch.astype(F32)).astype(BF16)

        @pl.when(jnp.logical_not(last))
        def _():
            @pl.when(unit >= 2)
            def _():
                pl.semaphore_wait(credit, 1)
            x_copy(unit).start()

        @pl.when(last)
        def _():
            for here, local, remote in out_parts(unit):
                @pl.when(here)
                def _():
                    local.start()

                @pl.when(jnp.logical_not(here))
                def _():
                    remote.start()

    feed(0)
    own_kv.start()
    own_q.start()
    own_o.start()

    for s in range(RING // 2):
        for copy in gate_copies(s):
            copy.start()

    @pl.when(west)
    def _():
        @pl.when(odd == 1)
        def _():
            pl.semaphore_wait(go, 1)

        gather_q.start()

        @pl.loop(0, PIECES)
        def _(p):
            relay_out(p).start()

    @pl.when(jnp.logical_not(west))
    def _():
        @pl.loop(0, PIECES)
        def _(p):
            relay_out(p).wait_recv()
            relay_back(p).start()

        @pl.loop(0, PIECES)
        def _(p):
            relay_back(p).wait_send()

        pl.semaphore_signal(ready, 1, device_id={'tp': other}, device_id_type=MESH)
        pl.semaphore_wait(ready, 1)

        @pl.when(odd == 1)
        def _():
            pl.semaphore_wait(go, 1)

        gather_q.start()
        gather_o.start()

    @pl.when(jnp.logical_not(first))
    def _():
        own_q.wait()
        gather_q.wait()
        gather_o_wait()

    feed(1)
    attend(0)

    @pl.loop(0, UNITS)
    def _(unit):
        u_copy(unit).wait_recv()

        @pl.when(unit + 2 < UNITS)
        def _():
            feed_wait(unit)
            feed(unit + 2)

        gate_up(unit, 0, FINISH_AT)

        @pl.when(unit > 0)
        def _():
            finish(unit - 1)

        gate_up(unit, FINISH_AT, ATTEND_AT)

        @pl.when(unit + 1 < UNITS)
        def _():
            attend(unit + 1)

        gate_up(unit, ATTEND_AT, GATE_BLOCKS)
        down(unit)

    finish(UNITS - 1)
    sends_wait(UNITS - 1)
    feed_wait(UNITS - 2)
    feed_wait(UNITS - 1)
    for s in range(2):
        u_copy(UNITS - 2 + s).wait_send()

    @pl.loop(0, DOWN_BLOCKS)
    def _(block):
        p_copy(UNITS - 1, block).wait_send()

    for m in range(MICRO):
        @pl.when(jnp.logical_not(last & (tp == m % 2)))
        def _():
            pltpu.make_async_copy(xout.at[pl.ds(0, OUT_ROWS), :], out.at[m], out_recv.at[m]).wait()


def solution(mesh):
    in_specs = (P('dp', None, 'tp', None), P('pp', None, None), P('pp', None, 'tp', None),
                P('pp', None, None, None), P('pp', None, None, None), P('pp', 'tp', None, None),
                P('pp', None, 'tp'), P('pp', None, 'tp'), P('pp', 'tp', None))
    out_spec = P('dp', None, ('tp', 'pp'), None)

    def stage_program(hidden_in, norm_gains, w_query, w_key, w_value, w_out, w_gate, w_up, w_down):
        cos, sin = rope_tables()
        wq = w_query[0].reshape(D, HEADS // 2 * HEAD)
        wkv = jnp.concatenate([w_key[0].reshape(D, KV * HEAD), w_value[0].reshape(D, KV * HEAD)], axis=1)
        wo = w_out[0].reshape(HEADS // 2 * HEAD, D)
        hbm = pl.BlockSpec(memory_space=pl.ANY)
        vmem = pl.BlockSpec(memory_space=pltpu.VMEM)
        dma = pltpu.SemaphoreType.DMA
        out = pl.pallas_call(
            kernel,
            out_shape=jax.ShapeDtypeStruct((MICRO, OUT_ROWS, D), BF16),
            in_specs=[hbm, vmem, vmem, vmem] + [hbm] * 6,
            out_specs=hbm,
            scratch_shapes=[
                pltpu.VMEM((D, HEADS * HEAD), BF16),
                pltpu.VMEM((D, 2 * KV * HEAD), BF16),
                pltpu.VMEM((HEADS * HEAD, D), BF16),
                pltpu.VMEM((ROWS, FF_LOCAL), BF16),
                pltpu.VMEM((RING, D, GATE_N), BF16),
                pltpu.VMEM((2, ROWS, D), BF16),
                pltpu.VMEM((SEQ, KV * HEAD), BF16),
                pltpu.VMEM((SEQ, KV * HEAD), BF16),
                pltpu.VMEM((2, CHUNK, D), BF16),
                pltpu.VMEM((2, CHUNK, D), BF16),
                pltpu.VMEM((CHUNK, D), BF16),
                pltpu.VMEM((2, CHUNK, D), BF16),
                pltpu.VMEM((CHUNK, D), F32),
                pltpu.VMEM((HEADS, CHUNK, HEAD), BF16),
                pltpu.VMEM((CHUNK, D), BF16),
                pltpu.VMEM((CHUNK, D), BF16),
                dma((3,)), dma((2,)), dma((2,)),
                dma((PIECES,)), dma((PIECES,)), dma((PIECES,)), dma((PIECES,)), pltpu.SemaphoreType.REGULAR, dma((RING,)), dma((2,)), dma((2,)),
                dma((DOWN_BLOCKS,)), dma((2, DOWN_BLOCKS)), dma((2,)), dma((2,)), dma((2,)),
                pltpu.SemaphoreType.REGULAR, pltpu.SemaphoreType.REGULAR,
                dma((MICRO,)), dma((2,)), dma,
            ],
            compiler_params=pltpu.CompilerParams(has_side_effects=True, vmem_limit_bytes=67043328),
            name='pipeline',
        )(hidden_in.reshape(MICRO, SEQ // 2, D), norm_gains[0], cos, sin, wq, wkv, wo, w_gate[0], w_up[0], w_down[0])
        return out.reshape(MICRO, 1, OUT_ROWS, D)

    return jax.shard_map(stage_program, mesh=mesh, in_specs=in_specs, out_specs=out_spec, check_vma=False)
```

```python
import functools

import jax
import jax.numpy as jnp
from jax import lax
from jax.experimental import pallas as pl
from jax.experimental.pallas import tpu as pltpu
from jax.sharding import PartitionSpec as P

WINDOW = 512
SOFTCAP = 50.0
ROPE_BASE = 10000.0
NORM_EPS = 1e-6
MESH = pl.DeviceIdType.MESH

D = 2048
HEAD = 256
HEADS = 8
KV = 2
GROUP = 4
FF_LOCAL = 8192
SEQ = 768
MICRO = 8
STAGES = 4
CHUNK = 192
CHUNKS = SEQ // CHUNK
ROWS = 2 * CHUNK
UNITS = (MICRO // 2) * CHUNKS
GATE_N = 512
GATE_BLOCKS = FF_LOCAL // GATE_N
DOWN_N = 512
DOWN_BLOCKS = D // DOWN_N
DOWN_K = FF_LOCAL // D
RING = 8
FINISH_AT = 4
ATTEND_AT = 8
STRIP = 64
OUT_ROWS = 96
PIECES = 8
F32 = jnp.float32
BF16 = jnp.bfloat16


def rope_tables():
    half = HEAD // 2
    frequency = jnp.power(ROPE_BASE, -2.0 * jnp.arange(half, dtype=F32) / HEAD)
    angle = jnp.arange(SEQ, dtype=F32)[:, None] * frequency[None, :]
    return jnp.cos(angle), jnp.sin(angle)


def dot(a, b):
    return jnp.dot(a, b, preferred_element_type=F32)


def kernel(hidden, gains, cos, sin, wq_hbm, wkv_hbm, wo_hbm, wg_hbm, wu_hbm, wd_hbm, out,
           wq, wkv, wo, hid, ring, ubuf, kcache, vcache, xbuf, x1buf, psend, precv, acc,
           qbuf, hbuf, xout,
           load_sem, gq_sem, go_sem, relay_send, relay_recv, back_send, back_recv, ready, ring_sem, u_send, u_recv, p_send, p_recv,
           x_recv, x_send, f_send, credit, go, out_recv, out_send, out_local):
    tp = lax.axis_index('tp')
    stage = lax.axis_index('pp')
    other = 1 - tp
    first = stage == 0
    last = stage == STAGES - 1
    odd = stage % 2
    half = HEADS // 2 * HEAD
    west = stage < STAGES // 2
    piece = half // PIECES

    def gate_copies(block):
        slot = 2 * lax.rem(block, RING // 2)
        cols = pl.ds(pl.multiple_of(block * GATE_N, GATE_N), GATE_N)
        return (pltpu.make_async_copy(wg_hbm.at[:, cols], ring.at[slot], ring_sem.at[slot]),
                pltpu.make_async_copy(wu_hbm.at[:, cols], ring.at[slot + 1], ring_sem.at[slot + 1]))

    def down_copies(block, parts):
        slot = DOWN_K * lax.rem(block, RING // DOWN_K)
        cols = pl.ds(pl.multiple_of(block * DOWN_N, DOWN_N), DOWN_N)
        return [pltpu.make_async_copy(
            wd_hbm.at[pl.ds(part * D if isinstance(part, int) else pl.multiple_of(part * D, D), D), cols],
            ring.at[slot + part], ring_sem.at[slot + part]) for part in parts]

    def feed(unit):
        micro = lax.div(unit, CHUNKS)
        chunk = lax.rem(unit, CHUNKS)
        slot = lax.rem(unit, 2)

        @pl.when(first & (lax.div(chunk, 2) == tp))
        def _():
            rows = pl.ds(pl.multiple_of(lax.rem(chunk, 2) * CHUNK, CHUNK), CHUNK)
            pltpu.make_async_copy(hidden.at[2 * micro + tp, rows, :], xbuf.at[slot], x_recv.at[slot]).start()
            pltpu.make_async_remote_copy(
                hidden.at[2 * micro + other, rows, :], xbuf.at[slot], f_send.at[slot], x_recv.at[slot],
                device_id={'tp': other}, device_id_type=MESH).start()

    def feed_wait(unit):
        chunk = lax.rem(unit, CHUNKS)
        slot = lax.rem(unit, 2)

        @pl.when(first & (lax.div(chunk, 2) == tp))
        def _():
            pltpu.make_async_remote_copy(
                hidden.at[0, pl.ds(0, CHUNK), :], xbuf.at[slot], f_send.at[slot], x_recv.at[slot],
                device_id={'tp': other}, device_id_type=MESH).wait_send()

    gather_q = pltpu.make_async_remote_copy(
        wq_hbm, wq.at[:, pl.ds(pl.multiple_of(tp * half, half), half)], gq_sem.at[0], gq_sem.at[1],
        device_id={'tp': other}, device_id_type=MESH)
    gather_o = pltpu.make_async_remote_copy(
        wo_hbm, wo.at[pl.ds(pl.multiple_of(tp * half, half), half), :], go_sem.at[0], go_sem.at[1],
        device_id={'tp': other}, device_id_type=MESH)
    own_q = pltpu.make_async_copy(wq_hbm, wq.at[:, pl.ds(pl.multiple_of(tp * half, half), half)], load_sem.at[0])
    own_o = pltpu.make_async_copy(wo_hbm, wo.at[pl.ds(pl.multiple_of(tp * half, half), half), :], load_sem.at[1])
    own_kv = pltpu.make_async_copy(wkv_hbm, wkv, load_sem.at[2])

    def relay_out(p):
        rows = pl.ds(pl.multiple_of(p * piece, piece), piece)
        there = pl.ds(pl.multiple_of(tp * half + p * piece, piece), piece)
        return pltpu.make_async_remote_copy(
            wo_hbm.at[rows, :], wo.at[there, :], relay_send.at[p], relay_recv.at[p],
            device_id={'tp': other, 'pp': stage + STAGES // 2}, device_id_type=MESH)

    def relay_back(p):
        rows = pl.ds(pl.multiple_of(other * half + p * piece, piece), piece)
        return pltpu.make_async_remote_copy(
            wo.at[rows, :], wo.at[rows, :], back_send.at[p], back_recv.at[p],
            device_id={'pp': stage - STAGES // 2}, device_id_type=MESH)

    def gather_o_wait():
        own_o.wait()

        @pl.when(west)
        def _():
            @pl.loop(0, PIECES)
            def _(p):
                relay_out(p).wait_send()
                relay_back(p).wait_recv()

        @pl.when(jnp.logical_not(west))
        def _():
            gather_o.wait()

        @pl.when(odd == 0)
        def _():
            pl.semaphore_signal(go, 1, device_id={'pp': stage + 1}, device_id_type=MESH)

    def u_copy(unit):
        slot = lax.rem(unit, 2)
        return pltpu.make_async_remote_copy(
            ubuf.at[slot, pl.ds(0, CHUNK), :], ubuf.at[slot, pl.ds(CHUNK, CHUNK), :], u_send.at[slot], u_recv.at[slot],
            device_id={'tp': other}, device_id_type=MESH)

    def p_copy(unit, block):
        slot = lax.rem(unit, 2)
        cols = pl.ds(pl.multiple_of(block * DOWN_N, DOWN_N), DOWN_N)
        return pltpu.make_async_remote_copy(
            psend.at[:, cols], precv.at[slot, :, cols], p_send.at[block], p_recv.at[slot, block],
            device_id={'tp': other}, device_id_type=MESH)

    def x_copy(unit):
        slot = lax.rem(unit, 2)
        return pltpu.make_async_remote_copy(
            xout, xbuf.at[slot], x_send.at[slot], x_recv.at[slot],
            device_id={'pp': stage + 1}, device_id_type=MESH)

    def out_parts(unit):
        micro = 2 * lax.div(unit, CHUNKS) + tp
        chunk = lax.rem(unit, CHUNKS)
        to_tp = lax.div(chunk, 2)
        parts = []
        for t in range(2):
            to_pp = lax.rem(chunk, 2) * 2 + t
            here = (to_tp == tp) & (to_pp == STAGES - 1)
            rows = pl.ds(t * OUT_ROWS, OUT_ROWS)
            local = pltpu.make_async_copy(xout.at[rows, :], out.at[micro], out_local)
            remote = pltpu.make_async_remote_copy(
                xout.at[rows, :], out.at[micro], out_send.at[t], out_recv.at[micro],
                device_id={'tp': to_tp, 'pp': to_pp}, device_id_type=MESH)
            parts.append((here, local, remote))
        return parts

    def sends_wait(unit):
        @pl.when(jnp.logical_not(last))
        def _():
            x_copy(unit).wait_send()

        @pl.when(last)
        def _():
            for here, local, remote in out_parts(unit):
                @pl.when(here)
                def _():
                    local.wait()

                @pl.when(jnp.logical_not(here))
                def _():
                    remote.wait_send()

    def normed(values, gain_row):
        mean_sq = jnp.mean(values * values, axis=-1, keepdims=True)
        return (values * lax.rsqrt(mean_sq + NORM_EPS) * (1.0 + gains[pl.ds(gain_row, 1), :])).astype(BF16)

    def attention(chunk, n):
        base = chunk * CHUNK
        row = lax.broadcasted_iota(jnp.int32, (GROUP, CHUNK, n), 1).reshape(GROUP * CHUNK, n) + base
        col = lax.broadcasted_iota(jnp.int32, (GROUP * CHUNK, n), 1)
        offset = row - col
        reach = jnp.where(odd == 0, WINDOW, SEQ)
        allowed = (offset >= 0) & (offset < reach)
        for g in range(KV):
            q = qbuf[pl.ds(g * GROUP, GROUP)].reshape(GROUP * CHUNK, HEAD)
            k = kcache[pl.ds(0, n), g * HEAD:(g + 1) * HEAD]
            v = vcache[pl.ds(0, n), g * HEAD:(g + 1) * HEAD]
            s = lax.dot_general(q, k, (((1,), (1,)), ((), ())), preferred_element_type=F32)
            s = SOFTCAP * jnp.tanh(s * (HEAD ** -0.5 / SOFTCAP))
            e = jnp.where(allowed, jnp.exp(s), 0.0)
            p = (e / jnp.sum(e, axis=-1, keepdims=True)).astype(BF16)
            o = dot(p, v).astype(BF16)
            for h in range(GROUP):
                hbuf[:, (g * GROUP + h) * HEAD:(g * GROUP + h + 1) * HEAD] = o[h * CHUNK:(h + 1) * CHUNK, :]

    def attend(unit):
        chunk = lax.rem(unit, CHUNKS)
        slot = lax.rem(unit, 2)
        pltpu.make_async_copy(xout, xbuf.at[slot], x_recv.at[slot]).wait()

        @pl.loop(0, CHUNK // STRIP)
        def _(r):
            rows = pl.ds(pl.multiple_of(r * STRIP, STRIP), STRIP)
            hbuf[rows, :] = normed(xbuf[slot, rows, :].astype(F32), 0)

        @pl.when(unit == 0)
        def _():
            own_kv.wait()

        positions = pl.ds(pl.multiple_of(chunk * CHUNK, CHUNK), CHUNK)

        def rotated(value):
            a, b = value[:, :HEAD // 2], value[:, HEAD // 2:]
            c, s = cos[positions, :], sin[positions, :]
            return (a * c - b * s).astype(BF16), (b * c + a * s).astype(BF16)

        kv = dot(hbuf[...], wkv[...])
        k = kv[:, :KV * HEAD]
        for g in range(KV):
            a, b = rotated(k[:, g * HEAD:(g + 1) * HEAD])
            kcache[positions, g * HEAD:g * HEAD + HEAD // 2] = a
            kcache[positions, g * HEAD + HEAD // 2:(g + 1) * HEAD] = b
        vcache[positions, :] = kv[:, KV * HEAD:].astype(BF16)

        @pl.when(first & (unit == 0))
        def _():
            own_q.wait()
            gather_q.wait()

        @pl.loop(0, KV)
        def _(g):
            q = dot(hbuf[...], wq[:, pl.ds(pl.multiple_of(g * GROUP * HEAD, GROUP * HEAD), GROUP * HEAD)])
            for t in range(GROUP):
                a, b = rotated(q[:, t * HEAD:(t + 1) * HEAD])
                qbuf[g * GROUP + t, :, :HEAD // 2] = a
                qbuf[g * GROUP + t, :, HEAD // 2:] = b

        for c in range(CHUNKS):
            @pl.when(chunk == c)
            def _():
                attention(c, (c + 1) * CHUNK)

        @pl.when(first & (unit == 0))
        def _():
            gather_o_wait()

        @pl.loop(0, D // 1024)
        def _(n):
            cols = pl.ds(pl.multiple_of(n * 1024, 1024), 1024)
            acc[:, cols] = dot(hbuf[...], wo[:, cols])

        @pl.when(unit >= 2)
        def _():
            u_copy(unit).wait_send()

        @pl.loop(0, CHUNK // STRIP)
        def _(r):
            rows = pl.ds(pl.multiple_of(r * STRIP, STRIP), STRIP)
            branch = normed(acc[rows, :].astype(BF16).astype(F32), 1)
            x1 = (xbuf[slot, rows, :].astype(F32) + branch.astype(F32)).astype(BF16)
            x1buf[slot, rows, :] = x1
            ubuf[slot, rows, :] = normed(x1.astype(F32), 2)

        u_copy(unit).start()

        @pl.when(jnp.logical_not(first) & (unit < UNITS - 2))
        def _():
            pl.semaphore_signal(credit, 1, device_id={'pp': stage - 1}, device_id_type=MESH)

    def gate_up(unit, pair):
        slot = lax.rem(unit, 2)
        at = 4 * lax.rem(pair, RING // 4)
        for t in range(2):
            for copy in gate_copies(2 * pair + t):
                copy.wait()
        for t in range(2):
            gate = dot(ubuf[slot], ring[at + 2 * t])
            up = dot(ubuf[slot], ring[at + 2 * t + 1])
            cols = pl.ds(pl.multiple_of((2 * pair + t) * GATE_N, GATE_N), GATE_N)
            hid[:, cols] = (jax.nn.gelu(gate, approximate=True) * up).astype(BF16)
        ahead = pair + RING // 4

        @pl.when(ahead < GATE_BLOCKS // 2)
        def _():
            for t in range(2):
                for copy in gate_copies(2 * ahead + t):
                    copy.start()

        @pl.when(ahead >= GATE_BLOCKS // 2)
        def _():
            for copy in down_copies(ahead - GATE_BLOCKS // 2, range(DOWN_K)):
                copy.start()

    def down(unit):
        @pl.loop(0, DOWN_BLOCKS)
        def _(block):
            cols = pl.ds(pl.multiple_of(block * DOWN_N, DOWN_N), DOWN_N)
            at = DOWN_K * lax.rem(block, RING // DOWN_K)

            @pl.when(unit > 0)
            def _():
                p_copy(unit, block).wait_send()

            for copy in down_copies(block, range(DOWN_K)):
                copy.wait()
            part = dot(hid[:, :D], ring[at])
            for k in range(1, DOWN_K):
                part = part + dot(hid[:, k * D:(k + 1) * D], ring[at + k])
            psend[:, cols] = part[CHUNK:, :].astype(BF16)
            acc[:, cols] = part[:CHUNK, :]
            p_copy(unit, block).start()
            ahead = block + RING // DOWN_K

            @pl.when(ahead < DOWN_BLOCKS)
            def _():
                for copy in down_copies(ahead, range(DOWN_K)):
                    copy.start()

            @pl.when((ahead >= DOWN_BLOCKS) & (unit + 1 < UNITS))
            def _():
                for t in range(2):
                    for copy in gate_copies((ahead - DOWN_BLOCKS) * 2 + t):
                        copy.start()

    def finish(unit):
        slot = lax.rem(unit, 2)

        @pl.when(unit > 0)
        def _():
            sends_wait(unit - 1)

        @pl.loop(0, DOWN_BLOCKS)
        def _(block):
            p_copy(unit, block).wait_recv()

        @pl.loop(0, CHUNK // STRIP)
        def _(r):
            rows = pl.ds(pl.multiple_of(r * STRIP, STRIP), STRIP)
            total = (acc[rows, :] + precv[slot, rows, :].astype(F32)).astype(BF16)
            branch = normed(total.astype(F32), 3)
            xout[rows, :] = (x1buf[slot, rows, :].astype(F32) + branch.astype(F32)).astype(BF16)

        @pl.when(jnp.logical_not(last))
        def _():
            @pl.when(unit >= 2)
            def _():
                pl.semaphore_wait(credit, 1)
            x_copy(unit).start()

        @pl.when(last)
        def _():
            for here, local, remote in out_parts(unit):
                @pl.when(here)
                def _():
                    local.start()

                @pl.when(jnp.logical_not(here))
                def _():
                    remote.start()

    feed(0)
    own_kv.start()
    own_q.start()
    own_o.start()

    for s in range(RING // 2):
        for copy in gate_copies(s):
            copy.start()

    @pl.when(west)
    def _():
        @pl.when(odd == 1)
        def _():
            pl.semaphore_wait(go, 1)

        gather_q.start()

        @pl.loop(0, PIECES)
        def _(p):
            relay_out(p).start()

    @pl.when(jnp.logical_not(west))
    def _():
        @pl.loop(0, PIECES)
        def _(p):
            relay_out(p).wait_recv()
            relay_back(p).start()

        @pl.loop(0, PIECES)
        def _(p):
            relay_back(p).wait_send()

        pl.semaphore_signal(ready, 1, device_id={'tp': other}, device_id_type=MESH)
        pl.semaphore_wait(ready, 1)

        @pl.when(odd == 1)
        def _():
            pl.semaphore_wait(go, 1)

        gather_q.start()
        gather_o.start()

    @pl.when(jnp.logical_not(first))
    def _():
        own_q.wait()
        gather_q.wait()
        gather_o_wait()

    feed(1)
    attend(0)

    @pl.loop(0, UNITS)
    def _(unit):
        u_copy(unit).wait_recv()

        @pl.when(unit + 2 < UNITS)
        def _():
            feed_wait(unit)
            feed(unit + 2)

        @pl.loop(0, GATE_BLOCKS // 2)
        def _(pair):
            @pl.when((2 * pair == FINISH_AT) & (unit > 0))
            def _():
                finish(unit - 1)

            @pl.when((2 * pair == ATTEND_AT) & (unit + 1 < UNITS))
            def _():
                attend(unit + 1)

            gate_up(unit, pair)

        down(unit)

    finish(UNITS - 1)
    sends_wait(UNITS - 1)
    feed_wait(UNITS - 2)
    feed_wait(UNITS - 1)
    for s in range(2):
        u_copy(UNITS - 2 + s).wait_send()

    @pl.loop(0, DOWN_BLOCKS)
    def _(block):
        p_copy(UNITS - 1, block).wait_send()

    for m in range(MICRO):
        @pl.when(jnp.logical_not(last & (tp == m % 2)))
        def _():
            pltpu.make_async_copy(xout.at[pl.ds(0, OUT_ROWS), :], out.at[m], out_recv.at[m]).wait()


def solution(mesh):
    in_specs = (P('dp', None, 'tp', None), P('pp', None, None), P('pp', None, 'tp', None),
                P('pp', None, None, None), P('pp', None, None, None), P('pp', 'tp', None, None),
                P('pp', None, 'tp'), P('pp', None, 'tp'), P('pp', 'tp', None))
    out_spec = P('dp', None, ('tp', 'pp'), None)

    def stage_program(hidden_in, norm_gains, w_query, w_key, w_value, w_out, w_gate, w_up, w_down):
        cos, sin = rope_tables()
        wq = w_query[0].reshape(D, HEADS // 2 * HEAD)
        wkv = jnp.concatenate([w_key[0].reshape(D, KV * HEAD), w_value[0].reshape(D, KV * HEAD)], axis=1)
        wo = w_out[0].reshape(HEADS // 2 * HEAD, D)
        hbm = pl.BlockSpec(memory_space=pl.ANY)
        vmem = pl.BlockSpec(memory_space=pltpu.VMEM)
        dma = pltpu.SemaphoreType.DMA
        out = pl.pallas_call(
            kernel,
            out_shape=jax.ShapeDtypeStruct((MICRO, OUT_ROWS, D), BF16),
            in_specs=[hbm, vmem, vmem, vmem] + [hbm] * 6,
            out_specs=hbm,
            scratch_shapes=[
                pltpu.VMEM((D, HEADS * HEAD), BF16),
                pltpu.VMEM((D, 2 * KV * HEAD), BF16),
                pltpu.VMEM((HEADS * HEAD, D), BF16),
                pltpu.VMEM((ROWS, FF_LOCAL), BF16),
                pltpu.VMEM((RING, D, GATE_N), BF16),
                pltpu.VMEM((2, ROWS, D), BF16),
                pltpu.VMEM((SEQ, KV * HEAD), BF16),
                pltpu.VMEM((SEQ, KV * HEAD), BF16),
                pltpu.VMEM((2, CHUNK, D), BF16),
                pltpu.VMEM((2, CHUNK, D), BF16),
                pltpu.VMEM((CHUNK, D), BF16),
                pltpu.VMEM((2, CHUNK, D), BF16),
                pltpu.VMEM((CHUNK, D), F32),
                pltpu.VMEM((HEADS, CHUNK, HEAD), BF16),
                pltpu.VMEM((CHUNK, D), BF16),
                pltpu.VMEM((CHUNK, D), BF16),
                dma((3,)), dma((2,)), dma((2,)),
                dma((PIECES,)), dma((PIECES,)), dma((PIECES,)), dma((PIECES,)), pltpu.SemaphoreType.REGULAR, dma((RING,)), dma((2,)), dma((2,)),
                dma((DOWN_BLOCKS,)), dma((2, DOWN_BLOCKS)), dma((2,)), dma((2,)), dma((2,)),
                pltpu.SemaphoreType.REGULAR, pltpu.SemaphoreType.REGULAR,
                dma((MICRO,)), dma((2,)), dma,
            ],
            compiler_params=pltpu.CompilerParams(has_side_effects=True, vmem_limit_bytes=67043328),
            name='pipeline',
        )(hidden_in.reshape(MICRO, SEQ // 2, D), norm_gains[0], cos, sin, wq, wkv, wo, w_gate[0], w_up[0], w_down[0])
        return out.reshape(MICRO, 1, OUT_ROWS, D)

    return jax.shard_map(stage_program, mesh=mesh, in_specs=in_specs, out_specs=out_spec, check_vma=False)
```
